32 devices in a mesh: row: 8 (over y, x, core), col: 4 (over z).
Axes of the slice: x: 2, y: 2, z: 4, core: 2. Of those that a mesh axis runs over, the one named last changes fastest.
Arguments:
- tokens: bfloat16 [256, 8192], P('row', 'col'), may hold values from -6 to 6
- gate_codes: int32 [1024, 28672], P('col', 'row'), may hold values from -2147483648 to 2147483646
- up_codes: int32 [1024, 28672], P('col', 'row'), may hold values from -2147483648 to 2147483646
- down_codes: int32 [3584, 8192], P('row', 'col'), may hold values from -2147483648 to 2147483646
- gate_scales: bfloat16 [64, 28672], P('row'), may hold values from 0.0009994507 to 0.0049743652
- up_scales: bfloat16 [64, 28672], P('row'), may hold values from 0.0009994507 to 0.0049743652
- down_scales: bfloat16 [8192, 224], P('row'), may hold values from 0.00059890747 to 0.0029907227
Outputs:
- mixed: bfloat16 [256, 8192], P('row', 'col')
The draws below stay inside these ranges and needn't reach their ends.
Inputs may be any that keep to these rules, and one draw needn't show every extreme that they name: Every word of gate_codes, up_codes and down_codes is an arbitrary 32-bit pattern: all sixteen codes occur in every nibble position.
All inputs are finite; a program needn't handle non-finite values.
Results may differ from the reference program's by a relative error of at most 0.025.
Values may be sent and summed in bfloat16 or wider, within the bound.
A program may use at most 192 MiB of HBM per device.

```python
import math
import jax
import jax.numpy as jnp
from jax import lax

D = 8192
FF = 28672
GROUP = 128
TOKENS = 256
N_ROW = 8


def plant(drawn, rng, smallest, high):
    index_at = [jax.random.randint(jax.random.fold_in(rng, axis), (), 0, length) for axis, length in enumerate(drawn.shape)]
    main_axis = drawn.shape.index(max(drawn.shape))
    neighbour = index_at[:main_axis] + [(index_at[main_axis] + 1) % drawn.shape[main_axis]] + index_at[main_axis + 1:]
    return drawn.at[tuple(index_at)].set(smallest).at[tuple(neighbour)].set(high)


def level_of(rng, dims, pieces, least, high):
    def one(dim, blocks):
        draws = jax.random.uniform(jax.random.fold_in(jax.random.fold_in(rng, 6), dim), (blocks,), jnp.float32, least / len(pieces), high / len(pieces))
        return jnp.repeat(jnp.exp(draws), dims[dim] // blocks).reshape((-1,) + (1,) * (len(dims) - dim - 1))

    gain = one(*pieces[0])
    for cut in pieces[1:]:
        gain = gain * one(*cut)
    return gain


def gaussian(rng, extent, deviation, bound, shards=(), held_as=jnp.bfloat16):
    result = jax.random.normal(rng, extent, jnp.float32) * deviation
    if len(shards) > 0:
        result = level_of(rng, extent, shards, -0.22, 0.18) * result
    return jnp.clip(result, min=-bound, max=bound).astype(held_as)


def setup_inputs(seed: int = 0) -> dict:
    streams_of = jax.random.split(jax.random.key(seed), 8)
    return {
        "tokens": gaussian(streams_of[0], (TOKENS, D), 1.0, 6.0, ((0, 8), (1, 4))),
        "gate_codes": plant(jax.random.randint(streams_of[1], (D // 8, FF), -2147483648, 2147483647), jax.random.fold_in(streams_of[1], 1), -2147483648, 2147483646).astype(jnp.int32),
        "up_codes": plant(jax.random.randint(streams_of[2], (D // 8, FF), -2147483648, 2147483647), jax.random.fold_in(streams_of[2], 1), -2147483648, 2147483646).astype(jnp.int32),
        "down_codes": plant(jax.random.randint(streams_of[3], (FF // 8, D), -2147483648, 2147483647), jax.random.fold_in(streams_of[3], 1), -2147483648, 2147483646).astype(jnp.int32),
        "gate_scales": jnp.clip(jnp.exp(math.log(0.0049743652) - 1.6048472 * jax.random.uniform(streams_of[4], (D // GROUP, FF), jnp.float32) ** level_of(streams_of[4], (D // GROUP, FF), ((0, 8),), -0.2, 0.2)), 0.0009994507, 0.0049743652).astype(jnp.bfloat16),
        "up_scales": jnp.clip(jnp.exp(math.log(0.0049743652) - 1.6048472 * jax.random.uniform(streams_of[5], (D // GROUP, FF), jnp.float32) ** level_of(streams_of[5], (D // GROUP, FF), ((0, 8),), -0.2, 0.2)), 0.0009994507, 0.0049743652).astype(jnp.bfloat16),
        "down_scales": jnp.clip(jnp.exp(math.log(0.0029907227) - 1.6081632 * jax.random.uniform(streams_of[6], (D, FF // GROUP), jnp.float32) ** level_of(streams_of[6], (D, FF // GROUP), ((0, 8),), -0.2, 0.2)), 0.00059890747, 0.0029907227).astype(jnp.bfloat16),
    }


def unpack_codes(packed):
    nibbles = [jnp.bitwise_and(jnp.right_shift(packed, 4 * offset), 15) for offset in range(8)]
    stacked = jnp.stack(nibbles, axis=1)
    return stacked.reshape(packed.shape[0] * 8, packed.shape[1]) - 8


def dequantize_rows(packed, scale_rows, group_size):
    values = unpack_codes(packed).astype(jnp.float32)
    columns = values.shape[1]
    shaped = values.reshape(scale_rows.shape[0], group_size, columns) * scale_rows.astype(jnp.float32)[:, None, :]
    return shaped.reshape(values.shape[0], columns).astype(jnp.bfloat16)


def split_cols(array):
    return array.reshape(array.shape[0], N_ROW, array.shape[1] // N_ROW).transpose(1, 0, 2)


def reference(tokens, gate_codes, up_codes, down_codes, gate_scales, up_scales, down_scales):
    down_blocks = down_codes.reshape(N_ROW, down_codes.shape[0] // N_ROW, D)

    def one_block(running, inputs):
        gate_packed, up_packed, gate_scale, up_scale, down_packed, down_scale = inputs
        gate_sum = jnp.dot(tokens, dequantize_rows(gate_packed, gate_scale, GROUP), preferred_element_type=jnp.float32)
        up_sum = jnp.dot(tokens, dequantize_rows(up_packed, up_scale, GROUP), preferred_element_type=jnp.float32)
        hidden = (jax.nn.silu(gate_sum) * up_sum).astype(jnp.bfloat16)
        partial_value = jnp.dot(hidden, dequantize_rows(down_packed, down_scale.T, GROUP), preferred_element_type=jnp.float32).astype(jnp.bfloat16)
        return running + partial_value.astype(jnp.float32), None

    start_sum = jnp.zeros((tokens.shape[0], D), jnp.float32)
    running, unused = lax.scan(one_block, start_sum, (split_cols(gate_codes), split_cols(up_codes), split_cols(gate_scales), split_cols(up_scales), down_blocks, split_cols(down_scales)))
    return running.astype(jnp.bfloat16)
```

```python
import jax
import jax.numpy as jnp
from jax import lax
from jax.experimental import pallas as pl
from jax.experimental.pallas import tpu as pltpu
from jax.sharding import PartitionSpec as P

GROUP = 128
PACK = 8
SUB = GROUP // PACK


def tile_of(width, most):
    tile = (min(width, most) // 128) * 128
    while width % tile:
        tile -= 128
    return tile


def permutation():
    source = lax.broadcasted_iota(jnp.int32, (GROUP, GROUP), 0)
    target = lax.broadcasted_iota(jnp.int32, (GROUP, GROUP), 1)
    wanted = lax.rem(target, SUB) * PACK + lax.div(target, SUB)
    return (source == wanted).astype(jnp.bfloat16)


def permute_features(source_ref, target_ref):
    perm = permutation()
    for group in range(source_ref.shape[1] // GROUP):
        at = pl.ds(group * GROUP, GROUP)
        target_ref[:, at] = jnp.dot(
            source_ref[:, at], perm, preferred_element_type=jnp.float32
        ).astype(jnp.bfloat16)


def dequantize(codes_ref, scales_ref, dense_ref):
    def one(group, carry):
        word = codes_ref[pl.ds(pl.multiple_of(group * SUB, SUB), SUB), :] ^ jnp.int32(-2004318072)
        scale = scales_ref[pl.ds(group, 1), :]
        for k in range(PACK):
            code = word if k == PACK - 1 else jnp.left_shift(word, 28 - 4 * k)
            value = jnp.right_shift(code, 28).astype(jnp.float32)
            row = pl.multiple_of(group * GROUP + k * SUB, SUB)
            dense_ref[pl.ds(row, SUB), :] = (value * scale).astype(jnp.bfloat16)
        return carry

    lax.fori_loop(0, codes_ref.shape[0] // SUB, one, 0)


def up_kernel(tokens, gate, up, gate_scale, up_scale, out, moved, dense):
    @pl.when(pl.program_id(0) == 0)
    def _():
        permute_features(tokens, moved)

    for index, (codes, scale) in enumerate(((gate, gate_scale), (up, up_scale))):
        dequantize(codes, scale, dense.at[index])
        total = jnp.dot(moved[...], dense[index], preferred_element_type=jnp.float32)
        parts, _, rows, width = out.shape
        out[:, index] = total.astype(jnp.bfloat16).reshape(parts, rows, width)


def down_kernel(hidden, codes, scale, out, moved, dense):
    @pl.when(pl.program_id(0) == 0)
    def _():
        permute_features(hidden, moved)

    dequantize(codes, scale, dense)
    out[...] = jnp.dot(moved[...], dense[...], preferred_element_type=jnp.float32).astype(
        jnp.bfloat16
    )


PARAMS = dict(dimension_semantics=("arbitrary",), vmem_limit_bytes=58 * 1024 * 1024)


def project_up(tokens, gate, up, gate_scale, up_scale, parts):
    count, model = tokens.shape
    words, width = gate.shape
    groups = gate_scale.shape[0]
    tile = tile_of(width, 512)
    codes = pl.BlockSpec((words, tile), lambda i: (0, i))
    scales = pl.BlockSpec((groups, tile), lambda i: (0, i))
    return pl.pallas_call(
        up_kernel,
        grid=(width // tile,),
        in_specs=[pl.BlockSpec((count, model), lambda i: (0, 0)), codes, codes, scales, scales],
        out_specs=pl.BlockSpec((parts, 2, count // parts, tile), lambda i: (0, 0, 0, i)),
        out_shape=jax.ShapeDtypeStruct((parts, 2, count // parts, width), jnp.bfloat16),
        scratch_shapes=[
            pltpu.VMEM((count, model), jnp.bfloat16),
            pltpu.VMEM((2, model, tile), jnp.bfloat16),
        ],
        cost_estimate=pl.CostEstimate(
            flops=4 * count * model * width,
            bytes_accessed=8 * words * width,
            transcendentals=0,
        ),
        compiler_params=pltpu.CompilerParams(**PARAMS),
    )(tokens, gate, up, gate_scale, up_scale)


def project_down(hidden, codes, scale):
    count, units = hidden.shape
    words, width = codes.shape
    groups = scale.shape[0]
    tile = tile_of(width, 512)
    return pl.pallas_call(
        down_kernel,
        grid=(width // tile,),
        in_specs=[
            pl.BlockSpec((count, units), lambda i: (0, 0)),
            pl.BlockSpec((words, tile), lambda i: (0, i)),
            pl.BlockSpec((groups, tile), lambda i: (0, i)),
        ],
        out_specs=pl.BlockSpec((count, tile), lambda i: (0, i)),
        out_shape=jax.ShapeDtypeStruct((count, width), jnp.bfloat16),
        scratch_shapes=[
            pltpu.VMEM((count, units), jnp.bfloat16),
            pltpu.VMEM((units, tile), jnp.bfloat16),
        ],
        cost_estimate=pl.CostEstimate(
            flops=2 * count * units * width,
            bytes_accessed=4 * words * width,
            transcendentals=0,
        ),
        compiler_params=pltpu.CompilerParams(**PARAMS),
    )(hidden, codes, scale)


def per_device(tokens, gate_codes, up_codes, down_codes, gate_scales, up_scales, down_scales):
    parts = lax.axis_size("col")
    col = lax.axis_index("col")
    gate_local, up_local, down_local = (
        lax.all_to_all(scales, "row", split_axis=1, concat_axis=0, tiled=True)
        for scales in (gate_scales, up_scales, down_scales)
    )
    groups = gate_local.shape[0] // parts
    gate_part = lax.dynamic_slice_in_dim(gate_local, col * groups, groups, 0).astype(jnp.float32)
    up_part = lax.dynamic_slice_in_dim(up_local, col * groups, groups, 0).astype(jnp.float32)
    width = down_codes.shape[1]
    down_part = lax.dynamic_slice_in_dim(down_local, col * width, width, 0).T.astype(jnp.float32)
    gathered = lax.all_gather(tokens, "row", axis=0, tiled=True)
    sums = project_up(gathered, gate_codes, up_codes, gate_part, up_part, parts)
    mine = lax.psum_scatter(sums, "col", scatter_dimension=0, tiled=True)[0].astype(jnp.float32)
    hidden = (jax.nn.silu(mine[0]) * mine[1]).astype(jnp.bfloat16)
    hidden = lax.all_gather(hidden, "col", axis=0, tiled=True)
    partial = project_down(hidden, down_codes, down_part)
    return lax.psum_scatter(partial, "row", scatter_dimension=0, tiled=True)


def solution(mesh):
    placed = (
        P("row", "col"),
        P("col", "row"),
        P("col", "row"),
        P("row", "col"),
        P("row", None),
        P("row", None),
        P("row", None),
    )
    return jax.shard_map(
        per_device, mesh=mesh, in_specs=placed, out_specs=P("row", "col"), check_vma=False
    )
```

```python
import functools

import jax
import jax.numpy as jnp
from jax import lax
from jax.experimental import pallas as pl
from jax.experimental.pallas import tpu as pltpu
from jax.sharding import PartitionSpec as P

GROUP = 128
PACK = 8
SUB = GROUP // PACK


def tile_of(width, most):
    tile = (min(width, most) // 128) * 128
    while width % tile:
        tile -= 128
    return tile


def permutation():
    source = lax.broadcasted_iota(jnp.int32, (GROUP, GROUP), 0)
    target = lax.broadcasted_iota(jnp.int32, (GROUP, GROUP), 1)
    wanted = lax.rem(target, SUB) * PACK + lax.div(target, SUB)
    return (source == wanted).astype(jnp.bfloat16)


def permute_features(source_ref, target_ref):
    perm = permutation()
    for group in range(source_ref.shape[1] // GROUP):
        at = pl.ds(group * GROUP, GROUP)
        target_ref[:, at] = jnp.dot(
            source_ref[:, at], perm, preferred_element_type=jnp.float32
        ).astype(jnp.bfloat16)


def dequantize(codes_ref, scales_ref, dense_ref):
    def one(group, carry):
        word = codes_ref[pl.ds(pl.multiple_of(group * SUB, SUB), SUB), :] ^ jnp.int32(-2004318072)
        scale = scales_ref[pl.ds(group, 1), :]
        for k in range(PACK):
            code = word if k == PACK - 1 else jnp.left_shift(word, 28 - 4 * k)
            value = jnp.right_shift(code, 28).astype(jnp.float32)
            row = pl.multiple_of(group * GROUP + k * SUB, SUB)
            dense_ref[pl.ds(row, SUB), :] = (value * scale).astype(jnp.bfloat16)
        return carry

    lax.fori_loop(0, codes_ref.shape[0] // SUB, one, 0)


def up_kernel(tokens, gate, up, gate_scale, up_scale, out, moved, dense):
    @pl.when(pl.program_id(0) == 0)
    def _():
        permute_features(tokens, moved)

    for index, (codes, scale) in enumerate(((gate, gate_scale), (up, up_scale))):
        dequantize(codes, scale, dense.at[index])
        total = jnp.dot(moved[...], dense[index], preferred_element_type=jnp.float32)
        out[index] = total.astype(jnp.bfloat16)


def down_kernel(hidden, codes, scale, out, moved, dense):
    @pl.when(pl.program_id(0) == 0)
    def _():
        permute_features(hidden, moved)

    dequantize(codes, scale, dense)
    out[...] = jnp.dot(moved[...], dense[...], preferred_element_type=jnp.float32).astype(
        jnp.bfloat16
    )


PARAMS = dict(dimension_semantics=("arbitrary",), vmem_limit_bytes=58 * 1024 * 1024)


def project_up(tokens, gate, up, gate_scale, up_scale):
    count, model = tokens.shape
    words, width = gate.shape
    groups = gate_scale.shape[0]
    tile = tile_of(width, 512)
    codes = pl.BlockSpec((words, tile), lambda i: (0, i))
    scales = pl.BlockSpec((groups, tile), lambda i: (0, i))
    return pl.pallas_call(
        up_kernel,
        grid=(width // tile,),
        in_specs=[pl.BlockSpec((count, model), lambda i: (0, 0)), codes, codes, scales, scales],
        out_specs=pl.BlockSpec((2, count, tile), lambda i: (0, 0, i)),
        out_shape=jax.ShapeDtypeStruct((2, count, width), jnp.bfloat16),
        scratch_shapes=[
            pltpu.VMEM((count, model), jnp.bfloat16),
            pltpu.VMEM((2, model, tile), jnp.bfloat16),
        ],
        cost_estimate=pl.CostEstimate(
            flops=4 * count * model * width,
            bytes_accessed=8 * words * width,
            transcendentals=0,
        ),
        compiler_params=pltpu.CompilerParams(**PARAMS),
    )(tokens, gate, up, gate_scale, up_scale)


def project_down(hidden, codes, scale):
    count, units = hidden.shape
    words, width = codes.shape
    groups = scale.shape[0]
    tile = tile_of(width, 512)
    return pl.pallas_call(
        down_kernel,
        grid=(width // tile,),
        in_specs=[
            pl.BlockSpec((count, units), lambda i: (0, 0)),
            pl.BlockSpec((words, tile), lambda i: (0, i)),
            pl.BlockSpec((groups, tile), lambda i: (0, i)),
        ],
        out_specs=pl.BlockSpec((count, tile), lambda i: (0, i)),
        out_shape=jax.ShapeDtypeStruct((count, width), jnp.bfloat16),
        scratch_shapes=[
            pltpu.VMEM((count, units), jnp.bfloat16),
            pltpu.VMEM((units, tile), jnp.bfloat16),
        ],
        cost_estimate=pl.CostEstimate(
            flops=2 * count * units * width,
            bytes_accessed=4 * words * width,
            transcendentals=0,
        ),
        compiler_params=pltpu.CompilerParams(**PARAMS),
    )(hidden, codes, scale)


VMEM_REF = pl.BlockSpec(memory_space=pltpu.VMEM)
MESH = pl.DeviceIdType.MESH
DMA = pltpu.SemaphoreType.DMA
REMOTE = pltpu.CompilerParams(has_side_effects=True, vmem_limit_bytes=58 * 1024 * 1024)


def gather_kernel(
    rows, share, tokens, gate, up, down, all_tokens, gate_out, up_out, down_out,
    gate_got, up_got, down_got, token_send, token_recv, scale_send, scale_recv,
):
    row, col = lax.axis_index("row"), lax.axis_index("col")
    count, width = tokens.shape[0], gate_got.shape[2]
    home, slot = lax.div(row, share), lax.rem(row, share)
    mine = pl.ds(pl.multiple_of(row * count, count), count)

    def token_copy(step):
        return pltpu.make_async_remote_copy(
            src_ref=tokens,
            dst_ref=all_tokens.at[mine],
            send_sem=token_send.at[step],
            recv_sem=token_recv.at[step],
            device_id={"row": lax.rem(row + step, rows), "col": col},
            device_id_type=MESH,
        )

    def scale_copies(j, at, peer_row, peer_col):
        columns = pl.ds(pl.multiple_of((col * share + j) * width, 128), width)
        pairs = (
            (gate.at[:, columns], gate_got.at[at]),
            (up.at[:, columns], up_got.at[at]),
            (down.at[col * share + j], down_got.at[at]),
        )
        return pairs, [
            pltpu.make_async_remote_copy(
                src_ref=source,
                dst_ref=target,
                send_sem=scale_send.at[kind, j],
                recv_sem=scale_recv.at[kind, at],
                device_id={"row": peer_row, "col": peer_col},
                device_id_type=MESH,
            )
            for kind, (source, target) in enumerate(pairs)
        ]

    for j in range(share):
        peer = col * share + j
        pairs, copies = scale_copies(j, slot, peer, home)
        here = jnp.logical_and(peer == row, home == col)

        @pl.when(jnp.logical_not(here))
        def _():
            for copy in copies:
                copy.start()

        @pl.when(here)
        def _():
            for source, target in pairs:
                target[...] = source[...]

    for step in range(rows - 1, 0, -1):
        token_copy(step).start()
    all_tokens[mine] = tokens[...]

    other = lax.rem(row + 1, rows)
    for t in range(share):
        @pl.when(col * share + t != row)
        def _():
            for copy in scale_copies(0, t, other, col)[1]:
                copy.wait_recv()

    lines, span = gate_got.shape[1], down_got.shape[2]
    for t in range(share):
        gate_out[t * lines : (t + 1) * lines] = gate_got[t].astype(jnp.float32)
        up_out[t * lines : (t + 1) * lines] = up_got[t].astype(jnp.float32)
        down_out[:, t * span : (t + 1) * span] = down_got[t].astype(jnp.float32)
    for step in range(1, rows):
        token_copy(step).wait()
    for j in range(share):
        peer = col * share + j

        @pl.when(jnp.logical_not(jnp.logical_and(peer == row, home == col)))
        def _():
            for copy in scale_copies(j, slot, peer, home)[1]:
                copy.wait_send()


def gather(tokens, gate, up, down, rows, cols):
    count, model = tokens.shape
    lines = gate.shape[0]
    width = gate.shape[1] // rows
    groups, span = down.shape[0] // rows, down.shape[1]
    share = rows // cols
    down = down.reshape(rows, groups, span)
    return pl.pallas_call(
        functools.partial(gather_kernel, rows, share),
        in_specs=[VMEM_REF] * 4,
        out_specs=[VMEM_REF] * 4,
        out_shape=[
            jax.ShapeDtypeStruct((count * rows, model), jnp.bfloat16),
            jax.ShapeDtypeStruct((share * lines, width), jnp.float32),
            jax.ShapeDtypeStruct((share * lines, width), jnp.float32),
            jax.ShapeDtypeStruct((groups, share * span), jnp.float32),
        ],
        scratch_shapes=[
            pltpu.VMEM((share, lines, width), jnp.bfloat16),
            pltpu.VMEM((share, lines, width), jnp.bfloat16),
            pltpu.VMEM((share, groups, span), jnp.bfloat16),
            DMA((rows,)),
            DMA((rows,)),
            DMA((3, share)),
            DMA((3, share)),
        ],
        compiler_params=REMOTE,
        name="gather",
    )(tokens, gate, up, down)


def chain_kernel(cols, chunks, sums, hidden, got, sum_send, sum_recv, hid_send, hid_recv):
    col = lax.axis_index("col")
    last = cols - 1
    half = sums.shape[1] // 2
    depth = half // chunks
    before, after = jnp.maximum(col - 1, 0), jnp.minimum(col + 1, last)
    any_peer = jnp.where(col == last, col - 1, col + 1)
    sides = ((last, 0, before, after), (0, last, after, before))

    def rows_of(side, q):
        return pl.ds(side * half + q * depth, depth)

    def sum_copy(side, q, source, peer):
        return pltpu.make_async_remote_copy(
            src_ref=source,
            dst_ref=got.at[side, q],
            send_sem=sum_send.at[side, q],
            recv_sem=sum_recv.at[side, q],
            device_id={"col": peer},
            device_id_type=MESH,
        )

    def hid_copy(side, q, peer):
        return pltpu.make_async_remote_copy(
            src_ref=hidden.at[rows_of(side, q)],
            dst_ref=hidden.at[rows_of(side, q)],
            send_sem=hid_send.at[side, q],
            recv_sem=hid_recv.at[side, q],
            device_id={"col": peer},
            device_id_type=MESH,
        )

    for side, (first, end, down_peer, up_peer) in enumerate(sides):
        @pl.when(col == first)
        def _():
            for q in range(chunks):
                sum_copy(side, q, sums.at[:, rows_of(side, q)], down_peer).start()

    for q in range(chunks):
        for side, (first, end, down_peer, up_peer) in enumerate(sides):
            @pl.when(col != first)
            def _():
                sum_copy(side, q, got.at[side, q], any_peer).wait_recv()
                total = got[side, q].astype(jnp.float32) + sums[:, rows_of(side, q)].astype(
                    jnp.float32
                )

                @pl.when(col != end)
                def _():
                    got[side, q] = total.astype(jnp.bfloat16)
                    sum_copy(side, q, got.at[side, q], down_peer).start()

                @pl.when(col == end)
                def _():
                    value = jax.nn.silu(total[0]) * total[1]
                    hidden[rows_of(side, q)] = value.astype(jnp.bfloat16)
                    hid_copy(side, q, up_peer).start()

    for q in range(chunks):
        for side, (first, end, down_peer, up_peer) in enumerate(sides):
            @pl.when(col != end)
            def _():
                hid_copy(side, q, any_peer).wait_recv()

                @pl.when(col != first)
                def _():
                    hid_copy(side, q, up_peer).start()

    for q in range(chunks):
        for side, (first, end, down_peer, up_peer) in enumerate(sides):
            @pl.when(col != end)
            def _():
                sum_copy(side, q, got.at[side, q], any_peer).wait_send()

            @pl.when(col != first)
            def _():
                hid_copy(side, q, any_peer).wait_send()


def chain(sums, cols):
    _, count, width = sums.shape
    chunks = 8
    while count % (2 * 16 * chunks):
        chunks //= 2
    depth = count // (2 * chunks)
    return pl.pallas_call(
        functools.partial(chain_kernel, cols, chunks),
        in_specs=[VMEM_REF],
        out_specs=VMEM_REF,
        out_shape=jax.ShapeDtypeStruct((count, width), jnp.bfloat16),
        scratch_shapes=[
            pltpu.VMEM((2, chunks, 2, depth, width), jnp.bfloat16),
            DMA((2, chunks)),
            DMA((2, chunks)),
            DMA((2, chunks)),
            DMA((2, chunks)),
        ],
        compiler_params=REMOTE,
        name="chain",
    )(sums)


def scatter_kernel(rows, partial, out, got, send, recv):
    row = lax.axis_index("row")
    count = out.shape[0]

    def block(index):
        return pl.ds(pl.multiple_of(index * count, count), count)

    def copy(step):
        peer = lax.rem(row + step, rows)
        return pltpu.make_async_remote_copy(
            src_ref=partial.at[block(peer)],
            dst_ref=got.at[step - 1],
            send_sem=send.at[step - 1],
            recv_sem=recv.at[step - 1],
            device_id={"row": peer},
            device_id_type=MESH,
        )

    for step in range(rows - 1, 0, -1):
        copy(step).start()
    total = partial[block(row)].astype(jnp.float32)
    for step in range(rows - 1, 0, -1):
        copy(step).wait_recv()
        total = total + got[step - 1].astype(jnp.float32)
    out[...] = total.astype(jnp.bfloat16)
    for step in range(1, rows):
        copy(step).wait_send()


def scatter(partial, rows):
    count, width = partial.shape
    return pl.pallas_call(
        functools.partial(scatter_kernel, rows),
        in_specs=[VMEM_REF],
        out_specs=VMEM_REF,
        out_shape=jax.ShapeDtypeStruct((count // rows, width), jnp.bfloat16),
        scratch_shapes=[
            pltpu.VMEM((rows - 1, count // rows, width), jnp.bfloat16),
            DMA((rows - 1,)),
            DMA((rows - 1,)),
        ],
        compiler_params=REMOTE,
        name="scatter",
    )(partial)


def per_device(tokens, gate_codes, up_codes, down_codes, gate_scales, up_scales, down_scales):
    rows, cols = lax.axis_size("row"), lax.axis_size("col")
    gathered, gate_part, up_part, down_part = gather(
        tokens, gate_scales, up_scales, down_scales.T, rows, cols
    )
    sums = project_up(gathered, gate_codes, up_codes, gate_part, up_part)
    hidden = chain(sums, cols)
    return scatter(project_down(hidden, down_codes, down_part), rows)


def solution(mesh):
    placed = (
        P("row", "col"),
        P("col", "row"),
        P("col", "row"),
        P("row", "col"),
        P("row", None),
        P("row", None),
        P("row", None),
    )
    return jax.shard_map(
        per_device, mesh=mesh, in_specs=placed, out_specs=P("row", "col"), check_vma=False
    )
```

```python
import functools

import jax
import jax.numpy as jnp
from jax import lax
from jax.experimental import pallas as pl
from jax.experimental.pallas import tpu as pltpu
from jax.sharding import PartitionSpec as P

GROUP = 128
PACK = 8
SUB = GROUP // PACK


def tile_of(width, most):
    tile = (min(width, most) // 128) * 128
    while width % tile:
        tile -= 128
    return tile


def permutation():
    source = lax.broadcasted_iota(jnp.int32, (GROUP, GROUP), 0)
    target = lax.broadcasted_iota(jnp.int32, (GROUP, GROUP), 1)
    wanted = lax.rem(target, SUB) * PACK + lax.div(target, SUB)
    return (source == wanted).astype(jnp.bfloat16)


def permute_features(source_ref, target_ref):
    perm = permutation()
    for group in range(source_ref.shape[1] // GROUP):
        at = pl.ds(group * GROUP, GROUP)
        target_ref[:, at] = jnp.dot(
            source_ref[:, at], perm, preferred_element_type=jnp.float32
        ).astype(jnp.bfloat16)


def dequantize(codes_ref, scales_ref, dense_ref):
    def one(group, carry):
        word = codes_ref[pl.ds(pl.multiple_of(group * SUB, SUB), SUB), :] ^ jnp.int32(-2004318072)
        scale = scales_ref[pl.ds(group, 1), :]
        for k in range(PACK):
            code = word if k == PACK - 1 else jnp.left_shift(word, 28 - 4 * k)
            value = jnp.right_shift(code, 28).astype(jnp.float32)
            row = pl.multiple_of(group * GROUP + k * SUB, SUB)
            dense_ref[pl.ds(row, SUB), :] = (value * scale).astype(jnp.bfloat16)
        return carry

    lax.fori_loop(0, codes_ref.shape[0] // SUB, one, 0)


def up_kernel(tokens, gate, up, gate_scale, up_scale, out, moved, dense):
    @pl.when(pl.program_id(0) == 0)
    def _():
        permute_features(tokens, moved)

    for index, (codes, scale) in enumerate(((gate, gate_scale), (up, up_scale))):
        dequantize(codes, scale, dense.at[index])
        total = jnp.dot(moved[...], dense[index], preferred_element_type=jnp.float32)
        out[index] = total.astype(jnp.bfloat16)


def down_kernel(hidden, codes, scale, out, moved, dense):
    @pl.when(pl.program_id(0) == 0)
    def _():
        permute_features(hidden, moved)

    dequantize(codes, scale, dense)
    out[...] = jnp.dot(moved[...], dense[...], preferred_element_type=jnp.float32).astype(
        jnp.bfloat16
    )


PARAMS = dict(dimension_semantics=("arbitrary",), vmem_limit_bytes=58 * 1024 * 1024)


def project_up(tokens, gate, up, gate_scale, up_scale):
    count, model = tokens.shape
    words, width = gate.shape
    groups = gate_scale.shape[0]
    tile = tile_of(width, 512)
    codes = pl.BlockSpec((words, tile), lambda i: (0, i))
    scales = pl.BlockSpec((groups, tile), lambda i: (0, i))
    return pl.pallas_call(
        up_kernel,
        grid=(width // tile,),
        in_specs=[pl.BlockSpec((count, model), lambda i: (0, 0)), codes, codes, scales, scales],
        out_specs=pl.BlockSpec((2, count, tile), lambda i: (0, 0, i)),
        out_shape=jax.ShapeDtypeStruct((2, count, width), jnp.bfloat16),
        scratch_shapes=[
            pltpu.VMEM((count, model), jnp.bfloat16),
            pltpu.VMEM((2, model, tile), jnp.bfloat16),
        ],
        cost_estimate=pl.CostEstimate(
            flops=4 * count * model * width,
            bytes_accessed=8 * words * width,
            transcendentals=0,
        ),
        compiler_params=pltpu.CompilerParams(**PARAMS),
    )(tokens, gate, up, gate_scale, up_scale)


def project_down(hidden, codes, scale):
    count, units = hidden.shape
    words, width = codes.shape
    groups = scale.shape[0]
    tile = tile_of(width, 512)
    return pl.pallas_call(
        down_kernel,
        grid=(width // tile,),
        in_specs=[
            pl.BlockSpec((count, units), lambda i: (0, 0)),
            pl.BlockSpec((words, tile), lambda i: (0, i)),
            pl.BlockSpec((groups, tile), lambda i: (0, i)),
        ],
        out_specs=pl.BlockSpec((count, tile), lambda i: (0, i)),
        out_shape=jax.ShapeDtypeStruct((count, width), jnp.bfloat16),
        scratch_shapes=[
            pltpu.VMEM((count, units), jnp.bfloat16),
            pltpu.VMEM((units, tile), jnp.bfloat16),
        ],
        cost_estimate=pl.CostEstimate(
            flops=2 * count * units * width,
            bytes_accessed=4 * words * width,
            transcendentals=0,
        ),
        compiler_params=pltpu.CompilerParams(**PARAMS),
    )(hidden, codes, scale)


VMEM_REF = pl.BlockSpec(memory_space=pltpu.VMEM)
MESH = pl.DeviceIdType.MESH
DMA = pltpu.SemaphoreType.DMA
REMOTE = pltpu.CompilerParams(has_side_effects=True, vmem_limit_bytes=58 * 1024 * 1024)


def gather_kernel(
    rows, cols, share, tokens, gate, up, down, all_tokens, gate_out, up_out, down_out,
    gate_got, up_got, down_got, token_send, token_recv, scale_send, scale_recv,
):
    row, col = lax.axis_index("row"), lax.axis_index("col")
    count, width = tokens.shape[0], gate_got.shape[2]
    home, slot = lax.div(row, share), lax.rem(row, share)
    group = lax.rem(col - home + cols, cols)
    sibling = row + 1 - 2 * lax.rem(row, 2)

    def block(owner):
        return pl.ds(pl.multiple_of(owner * count, count), count)

    def token_copy(step, peer, source, owner):
        return pltpu.make_async_remote_copy(
            src_ref=source,
            dst_ref=all_tokens.at[block(owner)],
            send_sem=token_send.at[step],
            recv_sem=token_recv.at[step],
            device_id={"row": peer, "col": col},
            device_id_type=MESH,
        )

    def own(step):
        return token_copy(step, lax.rem(row + step, rows), tokens, row)

    def relay(step):
        owner = lax.rem(row - step + rows, rows)
        return token_copy(step + 1, sibling, all_tokens.at[block(owner)], owner)

    to_sibling = token_copy(1, sibling, tokens, row)

    def scale_copies(j, at, peer_row, peer_col):
        columns = pl.ds(pl.multiple_of((group * share + j) * width, 128), width)
        pairs = (
            (gate.at[:, columns], gate_got.at[at]),
            (up.at[:, columns], up_got.at[at]),
            (down.at[group * share + j], down_got.at[at]),
        )
        return pairs, [
            pltpu.make_async_remote_copy(
                src_ref=source,
                dst_ref=target,
                send_sem=scale_send.at[kind, j],
                recv_sem=scale_recv.at[kind, at],
                device_id={"row": peer_row, "col": peer_col},
                device_id_type=MESH,
            )
            for kind, (source, target) in enumerate(pairs)
        ]

    for j in range(share):
        peer = group * share + j
        pairs, copies = scale_copies(j, slot, peer, home)
        here = jnp.logical_and(peer == row, home == col)

        @pl.when(jnp.logical_not(here))
        def _():
            for copy in copies:
                copy.start()

        @pl.when(here)
        def _():
            for source, target in pairs:
                target[...] = source[...]

    for step in range(rows - 2, 0, -2):
        own(step).start()
    to_sibling.start()
    all_tokens[block(row)] = tokens[...]
    for step in range(rows - 2, 0, -2):
        own(step).wait_recv()
        relay(step).start()

    other = lax.rem(row + 1, rows)
    from_col = lax.rem(col + lax.div(row, share), cols)
    for t in range(share):
        @pl.when(jnp.logical_or(col * share + t != row, from_col != col))
        def _():
            for copy in scale_copies(0, t, other, col)[1]:
                copy.wait_recv()

    lines, span = gate_got.shape[1], down_got.shape[2]
    for t in range(share):
        gate_out[t * lines : (t + 1) * lines] = gate_got[t].astype(jnp.float32)
        up_out[t * lines : (t + 1) * lines] = up_got[t].astype(jnp.float32)
        down_out[:, t * span : (t + 1) * span] = down_got[t].astype(jnp.float32)
    to_sibling.wait()
    for step in range(2, rows, 2):
        own(step).wait_send()
        relay(step).wait()
    for j in range(share):
        peer = group * share + j

        @pl.when(jnp.logical_not(jnp.logical_and(peer == row, home == col)))
        def _():
            for copy in scale_copies(j, slot, peer, home)[1]:
                copy.wait_send()


def gather(tokens, gate, up, down, rows, cols):
    count, model = tokens.shape
    lines = gate.shape[0]
    width = gate.shape[1] // rows
    groups, span = down.shape[0] // rows, down.shape[1]
    share = rows // cols
    down = down.reshape(rows, groups, span)
    return pl.pallas_call(
        functools.partial(gather_kernel, rows, cols, share),
        in_specs=[VMEM_REF] * 4,
        out_specs=[VMEM_REF] * 4,
        out_shape=[
            jax.ShapeDtypeStruct((count * rows, model), jnp.bfloat16),
            jax.ShapeDtypeStruct((share * lines, width), jnp.float32),
            jax.ShapeDtypeStruct((share * lines, width), jnp.float32),
            jax.ShapeDtypeStruct((groups, share * span), jnp.float32),
        ],
        scratch_shapes=[
            pltpu.VMEM((share, lines, width), jnp.bfloat16),
            pltpu.VMEM((share, lines, width), jnp.bfloat16),
            pltpu.VMEM((share, groups, span), jnp.bfloat16),
            DMA((rows,)),
            DMA((rows,)),
            DMA((3, share)),
            DMA((3, share)),
        ],
        compiler_params=REMOTE,
        name="gather",
    )(tokens, gate, up, down)


def chain_kernel(cols, chunks, sums, hidden, got, sum_send, sum_recv, hid_send, hid_recv):
    col = lax.axis_index("col")
    last = cols - 1
    half = sums.shape[1] // 2
    depth = half // chunks
    before, after = jnp.maximum(col - 1, 0), jnp.minimum(col + 1, last)
    any_peer = jnp.where(col == last, col - 1, col + 1)
    sides = ((last, 0, before, after), (0, last, after, before))

    def rows_of(side, q):
        return pl.ds(pl.multiple_of(side * half + q * depth, depth), depth)

    def sum_copy(side, q, source, peer):
        return pltpu.make_async_remote_copy(
            src_ref=source,
            dst_ref=got.at[side, q],
            send_sem=sum_send.at[side, q],
            recv_sem=sum_recv.at[side, q],
            device_id={"col": peer},
            device_id_type=MESH,
        )

    def hid_copy(side, q, peer):
        return pltpu.make_async_remote_copy(
            src_ref=hidden.at[rows_of(side, q)],
            dst_ref=hidden.at[rows_of(side, q)],
            send_sem=hid_send.at[side, q],
            recv_sem=hid_recv.at[side, q],
            device_id={"col": peer},
            device_id_type=MESH,
        )

    for side, (first, end, down_peer, up_peer) in enumerate(sides):
        @pl.when(col == first)
        def _():
            for q in range(chunks):
                sum_copy(side, q, sums.at[:, rows_of(side, q)], down_peer).start()

    def sum_step(step, carry):
        for side, (first, end, down_peer, up_peer) in enumerate(sides):
            q = step - (jnp.abs(col - first) - 1)

            @pl.when((col != first) & (q >= 0) & (q < chunks))
            def _():
                sum_copy(side, q, got.at[side, q], any_peer).wait_recv()
                total = got[side, q].astype(jnp.float32) + sums[:, rows_of(side, q)].astype(
                    jnp.float32
                )

                @pl.when(col != end)
                def _():
                    got[side, q] = total.astype(jnp.bfloat16)
                    sum_copy(side, q, got.at[side, q], down_peer).start()

                @pl.when(col == end)
                def _():
                    value = jax.nn.silu(total[0]) * total[1]
                    hidden[rows_of(side, q)] = value.astype(jnp.bfloat16)
                    hid_copy(side, q, up_peer).start()
        return carry

    def hid_step(step, carry):
        for side, (first, end, down_peer, up_peer) in enumerate(sides):
            q = step - (jnp.abs(col - end) - 1)

            @pl.when((col != end) & (q >= 0) & (q < chunks))
            def _():
                hid_copy(side, q, any_peer).wait_recv()

                @pl.when(col != first)
                def _():
                    hid_copy(side, q, up_peer).start()
        return carry

    lax.fori_loop(0, chunks + cols - 2, sum_step, 0)
    lax.fori_loop(0, chunks + cols - 2, hid_step, 0)

    for q in range(chunks):
        for side, (first, end, down_peer, up_peer) in enumerate(sides):
            @pl.when(col != end)
            def _():
                sum_copy(side, q, got.at[side, q], any_peer).wait_send()

            @pl.when(col != first)
            def _():
                hid_copy(side, q, any_peer).wait_send()


def chain(sums, cols):
    _, count, width = sums.shape
    chunks = 8
    while count % (2 * 16 * chunks):
        chunks //= 2
    depth = count // (2 * chunks)
    return pl.pallas_call(
        functools.partial(chain_kernel, cols, chunks),
        in_specs=[VMEM_REF],
        out_specs=VMEM_REF,
        out_shape=jax.ShapeDtypeStruct((count, width), jnp.bfloat16),
        scratch_shapes=[
            pltpu.VMEM((2, chunks, 2, depth, width), jnp.bfloat16),
            DMA((2, chunks)),
            DMA((2, chunks)),
            DMA((2, chunks)),
            DMA((2, chunks)),
        ],
        compiler_params=REMOTE,
        name="chain",
    )(sums)


def scatter_kernel(rows, partial, out, got, send, recv):
    row = lax.axis_index("row")
    count = out.shape[0]

    def block(index):
        return pl.ds(pl.multiple_of(index * count, count), count)

    def copy(step):
        peer = lax.rem(row + step, rows)
        return pltpu.make_async_remote_copy(
            src_ref=partial.at[block(peer)],
            dst_ref=got.at[step - 1],
            send_sem=send.at[step - 1],
            recv_sem=recv.at[step - 1],
            device_id={"row": peer},
            device_id_type=MESH,
        )

    for step in range(rows - 1, 0, -1):
        copy(step).start()
    total = partial[block(row)].astype(jnp.float32)
    for step in range(rows - 1, 0, -1):
        copy(step).wait_recv()
        total = total + got[step - 1].astype(jnp.float32)
    out[...] = total.astype(jnp.bfloat16)
    for step in range(1, rows):
        copy(step).wait_send()


def scatter(partial, rows):
    count, width = partial.shape
    return pl.pallas_call(
        functools.partial(scatter_kernel, rows),
        in_specs=[VMEM_REF],
        out_specs=VMEM_REF,
        out_shape=jax.ShapeDtypeStruct((count // rows, width), jnp.bfloat16),
        scratch_shapes=[
            pltpu.VMEM((rows - 1, count // rows, width), jnp.bfloat16),
            DMA((rows - 1,)),
            DMA((rows - 1,)),
        ],
        compiler_params=REMOTE,
        name="scatter",
    )(partial)


def per_device(tokens, gate_codes, up_codes, down_codes, gate_scales, up_scales, down_scales):
    rows, cols = lax.axis_size("row"), lax.axis_size("col")
    gathered, gate_part, up_part, down_part = gather(
        tokens, gate_scales, up_scales, down_scales.T, rows, cols
    )
    sums = project_up(gathered, gate_codes, up_codes, gate_part, up_part)
    hidden = chain(sums, cols)
    return scatter(project_down(hidden, down_codes, down_part), rows)


def solution(mesh):
    placed = (
        P("row", "col"),
        P("col", "row"),
        P("col", "row"),
        P("row", "col"),
        P("row", None),
        P("row", None),
        P("row", None),
    )
    return jax.shard_map(
        per_device, mesh=mesh, in_specs=placed, out_specs=P("row", "col"), check_vma=False
    )
```
